32 devices in a mesh: seq: 16 (over z, y, x), blk: 2 (over core).
Axes of the slice: x: 2, y: 2, z: 4, core: 2. Of those that a mesh axis runs over, the one named last changes fastest.
Arguments:
- query: bfloat16 [2048, 5120], P(('blk', 'seq')), may hold values from -139 to 139
- keys: bfloat16 [2048, 5120], P(('blk', 'seq')), may hold values from -4.5 to 4.5
- values: bfloat16 [2048, 5120], P(('blk', 'seq')), may hold values from -6 to 6
Outputs:
- attended: bfloat16 [2048, 5120], P(('blk', 'seq'))
The draws below stay inside these ranges and needn't reach their ends.
All inputs are finite; a program needn't handle non-finite values.
Results may differ from the reference program's by a relative error of at most 0.008.
Values may be sent and summed in bfloat16 or wider, within the bound.
A program may use at most 64 MiB of HBM per device.

```python
import jax
import jax.numpy as jnp
from jax import lax

HEADS = 40
HEAD_DIM = 128
SEQ_LEN = 2048


def joint_draw(key):
    base = jax.random.fold_in(key, 7)
    first, second = jax.random.split(base, 2)
    shape = (SEQ_LEN, HEADS * HEAD_DIM)
    keys = jnp.clip(jax.random.normal(first, shape, jnp.float32), -4.5, 4.5)
    query = jnp.clip(jax.random.normal(second, shape, jnp.float32), -4.5, 4.5)
    return (query, keys)


def draw_query(key, part):
    return joint_draw(key)[0].astype(jnp.bfloat16)


def draw_keys(key, part):
    return joint_draw(key)[1].astype(jnp.bfloat16)


def level_of(own_key, shape, pieces, smallest, top_value):
    level = 1.0
    for axis_at, parts in pieces:
        heights = jax.random.uniform(jax.random.fold_in(jax.random.fold_in(own_key, 6), axis_at), (parts,), jnp.float32, smallest / len(pieces), top_value / len(pieces))
        level = level * jnp.repeat(jnp.exp(heights), shape[axis_at] // parts).reshape((-1,) + (1,) * (len(shape) - 1 - axis_at))
    return level


def scatter_about(rng, extent, scale, reach, cuts=(), held_as=jnp.bfloat16):
    factor_of = level_of(rng, extent, cuts, -0.22, 0.18) if cuts else 1.0
    values = jax.random.normal(rng, extent, jnp.float32) * scale * factor_of
    return jnp.minimum(jnp.maximum(values, -reach), reach).astype(held_as)


def setup_inputs(seed: int = 0) -> dict:
    splits = jax.random.split(jax.random.key(seed), 4)
    return {
        "query": draw_query(jax.random.fold_in(splits[3], 71), 0),
        "keys": draw_keys(jax.random.fold_in(splits[3], 71), 0),
        "values": scatter_about(splits[2], (SEQ_LEN, HEADS * HEAD_DIM), 1.0, 6.0, ((0, 32),)),
    }


def reference(query, keys, values):
    length = query.shape[0]
    width = HEAD_DIM
    rows = min(512, length)

    def heads_first(array):
        return jnp.transpose(array.reshape(length, HEADS, width), (1, 0, 2))

    def one_head(args):
        q_head, k_head, v_head = args

        def block(q_rows):
            scores = lax.dot_general(q_rows, k_head, (((1,), (1,)), ((), ())), preferred_element_type=jnp.float32) * (width ** -0.5)
            peak = jnp.max(scores, axis=1, keepdims=True)
            expo = jnp.exp(scores - peak)
            totals = jnp.sum(expo, axis=1)
            summed = jnp.dot(expo.astype(jnp.bfloat16), v_head, preferred_element_type=jnp.float32)
            return (summed / totals[:, None]).astype(jnp.bfloat16)

        return lax.map(block, q_head.reshape(length // rows, rows, width)).reshape(length, width)

    result = lax.map(one_head, (heads_first(query), heads_first(keys), heads_first(values)))
    return jnp.transpose(result, (1, 0, 2)).reshape(length, HEADS * width)
```

```python
import functools
import math

import jax
import jax.numpy as jnp
from jax import lax
from jax.experimental import pallas as pl
from jax.experimental.pallas import tpu as pltpu
from jax.sharding import PartitionSpec as P

HEADS = 40
MESH = pl.DeviceIdType.MESH


def send_order(groups):
    return list(range(groups - 1, 0, -1))


def kernel(
    groups, ranks, cores, per_group, width,
    q_in, k_in, v_in, out,
    q_buf, k_buf, v_buf, o_buf,
    send_sem, fwd_sem, o_send, q_sem, k_sem, v_sem, o_sem,
):
    tok = q_in.shape[0]
    me = lax.axis_index("seq")
    blk = lax.axis_index("blk")
    group = me // ranks
    rank = lax.rem(me, ranks)
    order = send_order(groups)
    mine = rank * cores + blk
    scale = width ** (-0.5) * math.log2(math.e)

    def columns(g, h):
        return pl.ds(pl.multiple_of((g * per_group + h) * width, width), width)

    def rows(g):
        return pl.ds(pl.multiple_of(g * tok, tok), tok)

    def spread(h, source, landing, index, recv):
        for offset in order:
            other = group ^ offset
            pltpu.make_async_remote_copy(
                src_ref=source.at[:, columns(other, h)],
                dst_ref=landing.at[index + (rows(group),)],
                send_sem=send_sem.at[h],
                recv_sem=recv,
                device_id={"seq": other * ranks + rank},
                device_id_type=MESH,
            ).start()
        pltpu.make_async_copy(
            source.at[:, columns(group, h)], landing.at[index + (rows(group),)], recv
        ).start()

    def issue(h, _):
        spread(h, k_in, k_buf, (h, mine), k_sem.at[h, mine])
        spread(h, v_in, v_buf, (h, mine), v_sem.at[h, mine])
        spread(h, q_in, q_buf, (h,), q_sem.at[h])
        return 0

    lax.fori_loop(0, per_group, issue, 0)

    def arrived(buf, sem):
        pltpu.make_async_copy(buf, buf, sem).wait()

    def forward(h, buf, sem, part, target):
        pltpu.make_async_remote_copy(
            src_ref=buf.at[h, part],
            dst_ref=buf.at[h, part],
            send_sem=fwd_sem.at[h],
            recv_sem=sem.at[h, part],
            device_id=target,
            device_id_type=MESH,
        ).start()

    def to_cores(h, buf, sem, part):
        for step in range(1, cores):
            forward(h, buf, sem, part, {"blk": lax.rem(blk + step, cores)})

    def to_ranks(h, buf, sem, part):
        for step in range(1, ranks):
            peer = group * ranks + lax.rem(rank + step, ranks)
            forward(h, buf, sem, part, {"seq": peer})

    def update(h, part, state):
        scores = lax.dot_general(
            q_buf[h], k_buf[h, part], (((1,), (1,)), ((), ())),
            preferred_element_type=jnp.float32,
        )
        peak = jnp.max(scores, axis=1, keepdims=True)
        if state is not None:
            peak = jnp.maximum(peak, state[0])
        expo = jnp.exp2((scores - peak) * scale)
        total = jnp.sum(expo, axis=1, keepdims=True)
        summed = jnp.dot(
            expo.astype(jnp.bfloat16), v_buf[h, part], preferred_element_type=jnp.float32
        )
        if state is not None:
            fade = jnp.exp2((state[0] - peak) * scale)
            total += fade * state[1]
            summed += fade * state[2]
        return (peak, total, summed)

    def head(h, _):
        for buf, sem in ((k_buf, k_sem), (v_buf, v_sem)):
            arrived(buf.at[h, mine], sem.at[h, mine])
            to_ranks(h, buf, sem, mine)
            to_cores(h, buf, sem, mine)
        arrived(q_buf.at[h], q_sem.at[h])
        state = update(h, mine, None)

        def take(part, state):
            arrived(k_buf.at[h, part], k_sem.at[h, part])
            arrived(v_buf.at[h, part], v_sem.at[h, part])
            return update(h, part, state)

        for step in range(1, cores):
            state = take(rank * cores + lax.rem(blk + step, cores), state)
        for hop in range(1, ranks):
            base = lax.rem(rank + hop, ranks) * cores
            for buf, sem in ((k_buf, k_sem), (v_buf, v_sem)):
                arrived(buf.at[h, base + blk], sem.at[h, base + blk])
                to_cores(h, buf, sem, base + blk)
            state = update(h, base + blk, state)
            for step in range(1, cores):
                state = take(base + lax.rem(blk + step, cores), state)

        o_buf[h] = (state[2] / state[1]).astype(o_buf.dtype)
        for offset in order:
            other = group ^ offset
            pltpu.make_async_remote_copy(
                src_ref=o_buf.at[h, rows(other)],
                dst_ref=out.at[:, columns(group, h)],
                send_sem=o_send.at[h],
                recv_sem=o_sem.at[h],
                device_id={"seq": other * ranks + rank},
                device_id_type=MESH,
            ).start()
        pltpu.make_async_copy(
            o_buf.at[h, rows(group)], out.at[:, columns(group, h)], o_sem.at[h]
        ).start()
        return 0

    lax.fori_loop(0, per_group, head, 0)

    away = pl.ds(0, (groups - 1) * tok)
    full = groups * tok

    def finish(h, _):
        for _ in range(3):
            arrived(q_buf.at[h, away], send_sem.at[h])
        arrived(q_buf.at[h, away], o_send.at[h])
        count = 2 * (ranks - 1 + ranks * (cores - 1))
        for _ in range(count):
            arrived(q_buf.at[h], fwd_sem.at[h])
        arrived(o_buf.at[h], o_sem.at[h])
        return 0

    del full
    lax.fori_loop(0, per_group, finish, 0)


def on_device(query, keys, values):
    seq = lax.axis_size("seq")
    cores = lax.axis_size("blk")
    tok, columns = query.shape
    width = columns // HEADS
    groups = math.gcd(seq, HEADS)
    ranks = seq // groups
    per_group = HEADS // groups
    parts = ranks * cores
    span = groups * tok
    dtype = query.dtype
    vmem = pl.BlockSpec(memory_space=pltpu.VMEM)
    dma = pltpu.SemaphoreType.DMA
    return pl.pallas_call(
        functools.partial(kernel, groups, ranks, cores, per_group, width),
        out_shape=jax.ShapeDtypeStruct(query.shape, dtype),
        in_specs=[vmem] * 3,
        out_specs=vmem,
        scratch_shapes=[
            pltpu.VMEM((per_group, span, width), dtype),
            pltpu.VMEM((per_group, parts, span, width), dtype),
            pltpu.VMEM((per_group, parts, span, width), dtype),
            pltpu.VMEM((per_group, span, width), dtype),
            dma((per_group,)),
            dma((per_group,)),
            dma((per_group,)),
            dma((per_group,)),
            dma((per_group, parts)),
            dma((per_group, parts)),
            dma((per_group,)),
        ],
        compiler_params=pltpu.CompilerParams(
            has_side_effects=True, vmem_limit_bytes=56 * 1024 * 1024
        ),
    )(query, keys, values)


def solution(mesh):
    spec = P(("blk", "seq"), None)
    return jax.shard_map(
        on_device, mesh=mesh, in_specs=(spec,) * 3, out_specs=spec, check_vma=False
    )
```

```python
import functools
import math

import jax
import jax.numpy as jnp
from jax import lax
from jax.experimental import pallas as pl
from jax.experimental.pallas import tpu as pltpu
from jax.sharding import PartitionSpec as P

HEADS = 40
MESH = pl.DeviceIdType.MESH


def send_order(groups):
    return list(range(groups - 1, 0, -1))


def kernel(
    groups, ranks, cores, per_group, width,
    q_in, k_in, v_in, out,
    q_buf, k_buf, v_buf, o_buf,
    send_sem, fwd_sem, o_send, q_sem, k_sem, v_sem, o_sem,
):
    tok = q_in.shape[0]
    me = lax.axis_index("seq")
    blk = lax.axis_index("blk")
    group = me // ranks
    rank = lax.rem(me, ranks)
    order = send_order(groups)
    mine = rank * cores + blk
    scale = width ** (-0.5) * math.log2(math.e)

    barrier = pltpu.get_barrier_semaphore()
    peers = [{"seq": (group ^ offset) * ranks + rank} for offset in order]
    peers += [
        {"seq": group * ranks + lax.rem(rank + step, ranks)} for step in range(1, ranks)
    ]
    peers += [{"blk": lax.rem(blk + step, cores)} for step in range(1, cores)]
    for peer in peers:
        pl.semaphore_signal(barrier, inc=1, device_id=peer, device_id_type=MESH)
    pl.semaphore_wait(barrier, len(peers))

    def columns(g, h):
        return pl.ds(pl.multiple_of((g * per_group + h) * width, width), width)

    def rows(g):
        return pl.ds(pl.multiple_of(g * tok, tok), tok)

    def spread(h, source, landing, index, recv):
        for offset in order:
            other = group ^ offset
            pltpu.make_async_remote_copy(
                src_ref=source.at[:, columns(other, h)],
                dst_ref=landing.at[index + (rows(group),)],
                send_sem=send_sem.at[h],
                recv_sem=recv,
                device_id={"seq": other * ranks + rank},
                device_id_type=MESH,
            ).start()
        pltpu.make_async_copy(
            source.at[:, columns(group, h)], landing.at[index + (rows(group),)], recv
        ).start()

    def issue_kv(h):
        spread(h, k_in, k_buf, (h, mine), k_sem.at[h, mine])
        spread(h, v_in, v_buf, (h, mine), v_sem.at[h, mine])

    def issue_q(h):
        spread(h, q_in, q_buf, (h,), q_sem.at[h])

    def arrived(buf, sem):
        pltpu.make_async_copy(buf, buf, sem).wait()

    def forward(h, buf, sem, part, target):
        pltpu.make_async_remote_copy(
            src_ref=buf.at[h, part],
            dst_ref=buf.at[h, part],
            send_sem=fwd_sem.at[h],
            recv_sem=sem.at[h, part],
            device_id=target,
            device_id_type=MESH,
        ).start()

    def to_cores(h, buf, sem, part):
        for step in range(1, cores):
            forward(h, buf, sem, part, {"blk": lax.rem(blk + step, cores)})

    def to_ranks(h, buf, sem, part):
        for step in range(1, ranks):
            peer = group * ranks + lax.rem(rank + step, ranks)
            forward(h, buf, sem, part, {"seq": peer})

    def update(h, part, state):
        scores = lax.dot_general(
            q_buf[h], k_buf[h, part], (((1,), (1,)), ((), ())),
            preferred_element_type=jnp.float32,
        )
        peak = jnp.max(scores, axis=1, keepdims=True)
        if state is not None:
            peak = jnp.maximum(peak, state[0])
        expo = jnp.exp2((scores - peak) * scale)
        total = jnp.sum(expo, axis=1, keepdims=True)
        summed = jnp.dot(
            expo.astype(jnp.bfloat16), v_buf[h, part], preferred_element_type=jnp.float32
        )
        if state is not None:
            fade = jnp.exp2((state[0] - peak) * scale)
            total += fade * state[1]
            summed += fade * state[2]
        return (peak, total, summed)

    def near(h):
        for buf, sem in ((k_buf, k_sem), (v_buf, v_sem)):
            arrived(buf.at[h, mine], sem.at[h, mine])
            to_ranks(h, buf, sem, mine)
            to_cores(h, buf, sem, mine)

    def far(h):
        for hop in range(1, ranks):
            part = lax.rem(rank + hop, ranks) * cores + blk
            for buf, sem in ((k_buf, k_sem), (v_buf, v_sem)):
                arrived(buf.at[h, part], sem.at[h, part])
                to_cores(h, buf, sem, part)

    def attend(h):
        arrived(q_buf.at[h], q_sem.at[h])
        state = update(h, mine, None)
        for hop in range(1, ranks):
            state = update(h, lax.rem(rank + hop, ranks) * cores + blk, state)
        for hop in range(ranks):
            base = lax.rem(rank + hop, ranks) * cores
            for step in range(1, cores):
                part = base + lax.rem(blk + step, cores)
                arrived(k_buf.at[h, part], k_sem.at[h, part])
                arrived(v_buf.at[h, part], v_sem.at[h, part])
                state = update(h, part, state)
        o_buf[h] = (state[2] / state[1]).astype(o_buf.dtype)

    def give(h):
        for offset in order:
            other = group ^ offset
            pltpu.make_async_remote_copy(
                src_ref=o_buf.at[h, rows(other)],
                dst_ref=out.at[:, columns(group, h)],
                send_sem=o_send.at[h],
                recv_sem=o_sem.at[h],
                device_id={"seq": other * ranks + rank},
                device_id_type=MESH,
            ).start()
        pltpu.make_async_copy(
            o_buf.at[h, rows(group)], out.at[:, columns(group, h)], o_sem.at[h]
        ).start()

    last = per_group - 1

    issue_kv(0)
    issue_q(0)
    if per_group > 1:
        issue_kv(1)
    near(0)

    def head(h, _):
        @pl.when(h + 2 <= last)
        def _():
            issue_kv(h + 2)

        @pl.when(h + 1 <= last)
        def _():
            issue_q(h + 1)
            near(h + 1)

        far(h)

        @pl.when(h >= 1)
        def _():
            give(h - 1)

        attend(h)
        return 0

    lax.fori_loop(0, per_group, head, 0)
    give(last)

    away = pl.ds(0, (groups - 1) * tok)

    def finish(h, _):
        for _ in range(3):
            arrived(q_buf.at[h, away], send_sem.at[h])
        arrived(q_buf.at[h, away], o_send.at[h])
        count = 2 * (ranks - 1 + ranks * (cores - 1))
        for _ in range(count):
            arrived(q_buf.at[h], fwd_sem.at[h])
        arrived(o_buf.at[h], o_sem.at[h])
        return 0

    lax.fori_loop(0, per_group, finish, 0)


def place(source, out, sem):
    copy = pltpu.make_async_copy(source, out, sem)
    copy.start()
    copy.wait()


def on_device(query, keys, values):
    seq = lax.axis_size("seq")
    cores = lax.axis_size("blk")
    tok, columns = query.shape
    width = columns // HEADS
    groups = math.gcd(seq, HEADS)
    ranks = seq // groups
    per_group = HEADS // groups
    parts = ranks * cores
    span = groups * tok
    dtype = query.dtype
    vmem = pl.BlockSpec(memory_space=pltpu.VMEM)
    dma = pltpu.SemaphoreType.DMA
    landed = pl.pallas_call(
        functools.partial(kernel, groups, ranks, cores, per_group, width),
        out_shape=jax.ShapeDtypeStruct(query.shape, dtype),
        in_specs=[pl.BlockSpec(memory_space=pl.ANY)] * 3,
        out_specs=vmem,
        scratch_shapes=[
            pltpu.VMEM((per_group, span, width), dtype),
            pltpu.VMEM((per_group, parts, span, width), dtype),
            pltpu.VMEM((per_group, parts, span, width), dtype),
            pltpu.VMEM((per_group, span, width), dtype),
            dma((per_group,)),
            dma((per_group,)),
            dma((per_group,)),
            dma((per_group,)),
            dma((per_group, parts)),
            dma((per_group, parts)),
            dma((per_group,)),
        ],
        compiler_params=pltpu.CompilerParams(
            collective_id=0,
            has_side_effects=True,
            vmem_limit_bytes=60 * 1024 * 1024,
        ),
    )(query, keys, values)
    return pl.pallas_call(
        place,
        out_shape=jax.ShapeDtypeStruct(query.shape, dtype),
        in_specs=[vmem],
        out_specs=pl.BlockSpec(memory_space=pl.ANY),
        scratch_shapes=[dma],
        compiler_params=pltpu.CompilerParams(vmem_limit_bytes=4 * 1024 * 1024),
    )(landed)


def solution(mesh):
    spec = P(("blk", "seq"), None)
    return jax.shard_map(
        on_device, mesh=mesh, in_specs=(spec,) * 3, out_specs=spec, check_vma=False
    )
```

```python
import functools
import math

import jax
import jax.numpy as jnp
from jax import lax
from jax.experimental import pallas as pl
from jax.experimental.pallas import tpu as pltpu
from jax.sharding import PartitionSpec as P

HEADS = 40
MESH = pl.DeviceIdType.MESH


def send_order(groups):
    return list(range(groups - 1, 0, -1))


def kernel(
    groups, ranks, cores, per_group, width,
    q_hbm, k_hbm, v_hbm, out,
    q_in, k_in, v_in, q_buf, k_buf, v_buf, o_buf,
    load_sem, send_sem, fwd_sem, o_send, q_sem, k_sem, v_sem, o_sem,
):
    tok = q_in.shape[0]
    me = lax.axis_index("seq")
    blk = lax.axis_index("blk")
    group = me // ranks
    rank = lax.rem(me, ranks)
    order = send_order(groups)
    mine = rank * cores + blk
    scale = width ** (-0.5) * math.log2(math.e)

    loads = [
        pltpu.make_async_copy(source, kept, load_sem.at[index])
        for index, (source, kept) in enumerate(
            ((k_hbm, k_in), (v_hbm, v_in), (q_hbm, q_in))
        )
    ]
    for load in loads:
        load.start()

    barrier = pltpu.get_barrier_semaphore()
    peers = [{"seq": (group ^ offset) * ranks + rank} for offset in order]
    peers += [
        {"seq": group * ranks + lax.rem(rank + step, ranks)} for step in range(1, ranks)
    ]
    peers += [{"blk": lax.rem(blk + step, cores)} for step in range(1, cores)]
    for peer in peers:
        pl.semaphore_signal(barrier, inc=1, device_id=peer, device_id_type=MESH)
    pl.semaphore_wait(barrier, len(peers))

    def columns(g, h):
        return pl.ds(pl.multiple_of((g * per_group + h) * width, width), width)

    def rows(g):
        return pl.ds(pl.multiple_of(g * tok, tok), tok)

    def spread(h, source, landing, index, recv):
        for offset in order:
            other = group ^ offset
            pltpu.make_async_remote_copy(
                src_ref=source.at[:, columns(other, h)],
                dst_ref=landing.at[index + (rows(group),)],
                send_sem=send_sem.at[h],
                recv_sem=recv,
                device_id={"seq": other * ranks + rank},
                device_id_type=MESH,
            ).start()
        pltpu.make_async_copy(
            source.at[:, columns(group, h)], landing.at[index + (rows(group),)], recv
        ).start()

    def issue_kv(h):
        spread(h, k_in, k_buf, (h, mine), k_sem.at[h, mine])
        spread(h, v_in, v_buf, (h, mine), v_sem.at[h, mine])

    def issue_q(h):
        spread(h, q_in, q_buf, (h,), q_sem.at[h])

    def arrived(buf, sem):
        pltpu.make_async_copy(buf, buf, sem).wait()

    def forward(h, buf, sem, part, target):
        pltpu.make_async_remote_copy(
            src_ref=buf.at[h, part],
            dst_ref=buf.at[h, part],
            send_sem=fwd_sem.at[h],
            recv_sem=sem.at[h, part],
            device_id=target,
            device_id_type=MESH,
        ).start()

    def to_cores(h, buf, sem, part):
        for step in range(1, cores):
            forward(h, buf, sem, part, {"blk": lax.rem(blk + step, cores)})

    def to_ranks(h, buf, sem, part):
        for step in range(1, ranks):
            peer = group * ranks + lax.rem(rank + step, ranks)
            forward(h, buf, sem, part, {"seq": peer})

    def update(h, part, state):
        scores = lax.dot_general(
            q_buf[h], k_buf[h, part], (((1,), (1,)), ((), ())),
            preferred_element_type=jnp.float32,
        )
        peak = jnp.max(scores, axis=1, keepdims=True)
        if state is not None:
            peak = jnp.maximum(peak, state[0])
        expo = jnp.exp2((scores - peak) * scale)
        total = jnp.sum(expo, axis=1, keepdims=True)
        summed = jnp.dot(
            expo.astype(jnp.bfloat16), v_buf[h, part], preferred_element_type=jnp.float32
        )
        if state is not None:
            fade = jnp.exp2((state[0] - peak) * scale)
            total += fade * state[1]
            summed += fade * state[2]
        return (peak, total, summed)

    def near(h):
        for buf, sem in ((k_buf, k_sem), (v_buf, v_sem)):
            arrived(buf.at[h, mine], sem.at[h, mine])
            to_ranks(h, buf, sem, mine)
            to_cores(h, buf, sem, mine)

    def far(h):
        for hop in range(1, ranks):
            part = lax.rem(rank + hop, ranks) * cores + blk
            for buf, sem in ((k_buf, k_sem), (v_buf, v_sem)):
                arrived(buf.at[h, part], sem.at[h, part])
                to_cores(h, buf, sem, part)

    def attend(h):
        arrived(q_buf.at[h], q_sem.at[h])
        state = update(h, mine, None)
        for hop in range(1, ranks):
            state = update(h, lax.rem(rank + hop, ranks) * cores + blk, state)
        for hop in range(ranks):
            base = lax.rem(rank + hop, ranks) * cores
            for step in range(1, cores):
                part = base + lax.rem(blk + step, cores)
                arrived(k_buf.at[h, part], k_sem.at[h, part])
                arrived(v_buf.at[h, part], v_sem.at[h, part])
                state = update(h, part, state)
        o_buf[h] = (state[2] / state[1]).astype(o_buf.dtype)

    def give(h):
        for offset in order:
            other = group ^ offset
            pltpu.make_async_remote_copy(
                src_ref=o_buf.at[h, rows(other)],
                dst_ref=out.at[:, columns(group, h)],
                send_sem=o_send.at[h],
                recv_sem=o_sem.at[h],
                device_id={"seq": other * ranks + rank},
                device_id_type=MESH,
            ).start()
        pltpu.make_async_copy(
            o_buf.at[h, rows(group)], out.at[:, columns(group, h)], o_sem.at[h]
        ).start()

    last = per_group - 1

    for load in loads:
        load.wait()
    issue_kv(0)
    issue_q(0)
    if per_group > 1:
        issue_kv(1)
    near(0)

    def head(h, _):
        @pl.when(h + 2 <= last)
        def _():
            issue_kv(h + 2)

        @pl.when(h + 1 <= last)
        def _():
            issue_q(h + 1)
            near(h + 1)

        far(h)

        @pl.when(h >= 1)
        def _():
            give(h - 1)

        attend(h)
        return 0

    lax.fori_loop(0, per_group, head, 0)
    give(last)

    away = pl.ds(0, (groups - 1) * tok)

    def finish(h, _):
        for _ in range(3):
            arrived(q_buf.at[h, away], send_sem.at[h])
        arrived(q_buf.at[h, away], o_send.at[h])
        count = 2 * (ranks - 1 + ranks * (cores - 1))
        for _ in range(count):
            arrived(q_buf.at[h], fwd_sem.at[h])
        arrived(o_buf.at[h], o_sem.at[h])
        return 0

    lax.fori_loop(0, per_group, finish, 0)


def place(source, out, sem):
    copy = pltpu.make_async_copy(source, out, sem)
    copy.start()
    copy.wait()


def on_device(query, keys, values):
    seq = lax.axis_size("seq")
    cores = lax.axis_size("blk")
    tok, columns = query.shape
    width = columns // HEADS
    groups = math.gcd(seq, HEADS)
    ranks = seq // groups
    per_group = HEADS // groups
    parts = ranks * cores
    span = groups * tok
    dtype = query.dtype
    vmem = pl.BlockSpec(memory_space=pltpu.VMEM)
    dma = pltpu.SemaphoreType.DMA
    held = (2 * parts + 2) * per_group * span * width * dtype.itemsize
    inputs = [
        pltpu.with_memory_space_constraint(array, pltpu.HBM)
        for array in (query, keys, values)
    ]
    landed = pl.pallas_call(
        functools.partial(kernel, groups, ranks, cores, per_group, width),
        out_shape=pltpu.VMEM(query.shape, dtype),
        in_specs=[pl.BlockSpec(memory_space=pl.ANY)] * 3,
        out_specs=vmem,
        scratch_shapes=[
            pltpu.VMEM(query.shape, dtype),
            pltpu.VMEM(query.shape, dtype),
            pltpu.VMEM(query.shape, dtype),
            pltpu.VMEM((per_group, span, width), dtype),
            pltpu.VMEM((per_group, parts, span, width), dtype),
            pltpu.VMEM((per_group, parts, span, width), dtype),
            pltpu.VMEM((per_group, span, width), dtype),
            dma((3,)),
            dma((per_group,)),
            dma((per_group,)),
            dma((per_group,)),
            dma((per_group,)),
            dma((per_group, parts)),
            dma((per_group, parts)),
            dma((per_group,)),
        ],
        compiler_params=pltpu.CompilerParams(
            collective_id=0,
            has_side_effects=True,
            vmem_limit_bytes=held + 12 * 1024 * 1024,
        ),
    )(*inputs)
    return pl.pallas_call(
        place,
        out_shape=jax.ShapeDtypeStruct(query.shape, dtype),
        in_specs=[vmem],
        out_specs=pl.BlockSpec(memory_space=pl.ANY),
        scratch_shapes=[dma],
        compiler_params=pltpu.CompilerParams(vmem_limit_bytes=4 * 1024 * 1024),
    )(landed)


def solution(mesh):
    spec = P(("blk", "seq"), None)
    return jax.shard_map(
        on_device, mesh=mesh, in_specs=(spec,) * 3, out_specs=spec, check_vma=False
    )
```

```python
import functools
import math

import jax
import jax.numpy as jnp
from jax import lax
from jax.experimental import pallas as pl
from jax.experimental.pallas import tpu as pltpu
from jax.sharding import PartitionSpec as P

HEADS = 40
MESH = pl.DeviceIdType.MESH


def send_order(groups):
    return sorted(range(1, groups), key=lambda o: (-(o % 4 >= 2), -o))


def kernel(
    groups, ranks, cores, per_group, width,
    q_hbm, k_hbm, v_hbm, out,
    q_in, k_in, v_in, q_buf, k_buf, v_buf, o_buf,
    load_sem, send_sem, fwd_sem, o_send, q_sem, k_sem, v_sem, o_sem,
):
    tok = q_in.shape[0]
    me = lax.axis_index("seq")
    blk = lax.axis_index("blk")
    group = me // ranks
    rank = lax.rem(me, ranks)
    order = send_order(groups)
    mine = rank * cores + blk
    scale = width ** (-0.5) * math.log2(math.e)

    loads = [
        pltpu.make_async_copy(source, kept, load_sem.at[index])
        for index, (source, kept) in enumerate(
            ((k_hbm, k_in), (v_hbm, v_in), (q_hbm, q_in))
        )
    ]
    for load in loads:
        load.start()

    barrier = pltpu.get_barrier_semaphore()
    peers = [{"seq": (group ^ offset) * ranks + rank} for offset in order]
    peers += [
        {"seq": group * ranks + lax.rem(rank + step, ranks)} for step in range(1, ranks)
    ]
    peers += [{"blk": lax.rem(blk + step, cores)} for step in range(1, cores)]
    for peer in peers:
        pl.semaphore_signal(barrier, inc=1, device_id=peer, device_id_type=MESH)
    pl.semaphore_wait(barrier, len(peers))

    def columns(g, h):
        return pl.ds(pl.multiple_of((g * per_group + h) * width, width), width)

    def rows(g):
        return pl.ds(pl.multiple_of(g * tok, tok), tok)

    def spread(h, source, landing, index, recv):
        for offset in order:
            other = group ^ offset
            pltpu.make_async_remote_copy(
                src_ref=source.at[:, columns(other, h)],
                dst_ref=landing.at[index + (rows(group),)],
                send_sem=send_sem.at[h],
                recv_sem=recv,
                device_id={"seq": other * ranks + rank},
                device_id_type=MESH,
            ).start()
        pltpu.make_async_copy(
            source.at[:, columns(group, h)], landing.at[index + (rows(group),)], recv
        ).start()

    def issue_kv(h):
        spread(h, k_in, k_buf, (h, mine), k_sem.at[h, mine])
        spread(h, v_in, v_buf, (h, mine), v_sem.at[h, mine])

    def issue_q(h):
        spread(h, q_in, q_buf, (h,), q_sem.at[h])

    def arrived(buf, sem):
        pltpu.make_async_copy(buf, buf, sem).wait()

    def forward(h, buf, sem, part, target):
        pltpu.make_async_remote_copy(
            src_ref=buf.at[h, part],
            dst_ref=buf.at[h, part],
            send_sem=fwd_sem.at[h],
            recv_sem=sem.at[h, part],
            device_id=target,
            device_id_type=MESH,
        ).start()

    def to_cores(h, buf, sem, part):
        for step in range(1, cores):
            forward(h, buf, sem, part, {"blk": lax.rem(blk + step, cores)})

    def to_ranks(h, buf, sem, part):
        for step in range(1, ranks):
            peer = group * ranks + lax.rem(rank + step, ranks)
            forward(h, buf, sem, part, {"seq": peer})

    def update(h, part, state):
        scores = lax.dot_general(
            q_buf[h], k_buf[h, part], (((1,), (1,)), ((), ())),
            preferred_element_type=jnp.float32,
        )
        peak = jnp.max(scores, axis=1, keepdims=True)
        if state is not None:
            peak = jnp.maximum(peak, state[0])
        expo = jnp.exp2((scores - peak) * scale)
        total = jnp.sum(expo, axis=1, keepdims=True)
        summed = jnp.dot(
            expo.astype(jnp.bfloat16), v_buf[h, part], preferred_element_type=jnp.float32
        )
        if state is not None:
            fade = jnp.exp2((state[0] - peak) * scale)
            total += fade * state[1]
            summed += fade * state[2]
        return (peak, total, summed)

    def near(h):
        for buf, sem in ((k_buf, k_sem), (v_buf, v_sem)):
            arrived(buf.at[h, mine], sem.at[h, mine])
            to_ranks(h, buf, sem, mine)
            to_cores(h, buf, sem, mine)

    def far(h):
        for hop in range(1, ranks):
            part = lax.rem(rank + hop, ranks) * cores + blk
            for buf, sem in ((k_buf, k_sem), (v_buf, v_sem)):
                arrived(buf.at[h, part], sem.at[h, part])
                to_cores(h, buf, sem, part)

    def attend(h):
        arrived(q_buf.at[h], q_sem.at[h])
        state = update(h, mine, None)
        for hop in range(1, ranks):
            state = update(h, lax.rem(rank + hop, ranks) * cores + blk, state)
        for hop in range(ranks):
            base = lax.rem(rank + hop, ranks) * cores
            for step in range(1, cores):
                part = base + lax.rem(blk + step, cores)
                arrived(k_buf.at[h, part], k_sem.at[h, part])
                arrived(v_buf.at[h, part], v_sem.at[h, part])
                state = update(h, part, state)
        o_buf[h] = (state[2] / state[1]).astype(o_buf.dtype)

    def give(h):
        for offset in order:
            other = group ^ offset
            pltpu.make_async_remote_copy(
                src_ref=o_buf.at[h, rows(other)],
                dst_ref=out.at[:, columns(group, h)],
                send_sem=o_send.at[h],
                recv_sem=o_sem.at[h],
                device_id={"seq": other * ranks + rank},
                device_id_type=MESH,
            ).start()
        pltpu.make_async_copy(
            o_buf.at[h, rows(group)], out.at[:, columns(group, h)], o_sem.at[h]
        ).start()

    last = per_group - 1

    loads[0].wait()
    loads[1].wait()
    issue_kv(0)
    loads[2].wait()
    issue_q(0)
    if per_group > 1:
        issue_kv(1)
    near(0)

    def head(h, _):
        @pl.when(h + 2 <= last)
        def _():
            issue_kv(h + 2)

        @pl.when(h + 1 <= last)
        def _():
            issue_q(h + 1)
            near(h + 1)

        @pl.when(h >= 1)
        def _():
            give(h - 1)

        far(h)

        attend(h)
        return 0

    lax.fori_loop(0, per_group, head, 0)
    give(last)

    away = pl.ds(0, (groups - 1) * tok)

    def finish(h, _):
        for _ in range(3):
            arrived(q_buf.at[h, away], send_sem.at[h])
        arrived(q_buf.at[h, away], o_send.at[h])
        count = 2 * (ranks - 1 + ranks * (cores - 1))
        for _ in range(count):
            arrived(q_buf.at[h], fwd_sem.at[h])
        arrived(o_buf.at[h], o_sem.at[h])
        return 0

    lax.fori_loop(0, per_group, finish, 0)


def place(source, out, sem):
    copy = pltpu.make_async_copy(source, out, sem)
    copy.start()
    copy.wait()


def on_device(query, keys, values):
    seq = lax.axis_size("seq")
    cores = lax.axis_size("blk")
    tok, columns = query.shape
    width = columns // HEADS
    groups = math.gcd(seq, HEADS)
    ranks = seq // groups
    per_group = HEADS // groups
    parts = ranks * cores
    span = groups * tok
    dtype = query.dtype
    vmem = pl.BlockSpec(memory_space=pltpu.VMEM)
    dma = pltpu.SemaphoreType.DMA
    held = (2 * parts + 2) * per_group * span * width * dtype.itemsize
    inputs = [
        pltpu.with_memory_space_constraint(array, pltpu.HBM)
        for array in (query, keys, values)
    ]
    landed = pl.pallas_call(
        functools.partial(kernel, groups, ranks, cores, per_group, width),
        out_shape=pltpu.VMEM(query.shape, dtype),
        in_specs=[pl.BlockSpec(memory_space=pl.ANY)] * 3,
        out_specs=vmem,
        scratch_shapes=[
            pltpu.VMEM(query.shape, dtype),
            pltpu.VMEM(query.shape, dtype),
            pltpu.VMEM(query.shape, dtype),
            pltpu.VMEM((per_group, span, width), dtype),
            pltpu.VMEM((per_group, parts, span, width), dtype),
            pltpu.VMEM((per_group, parts, span, width), dtype),
            pltpu.VMEM((per_group, span, width), dtype),
            dma((3,)),
            dma((per_group,)),
            dma((per_group,)),
            dma((per_group,)),
            dma((per_group,)),
            dma((per_group, parts)),
            dma((per_group, parts)),
            dma((per_group,)),
        ],
        compiler_params=pltpu.CompilerParams(
            collective_id=0,
            has_side_effects=True,
            vmem_limit_bytes=held + 12 * 1024 * 1024,
        ),
    )(*inputs)
    return pl.pallas_call(
        place,
        out_shape=jax.ShapeDtypeStruct(query.shape, dtype),
        in_specs=[vmem],
        out_specs=pl.BlockSpec(memory_space=pl.ANY),
        scratch_shapes=[dma],
        compiler_params=pltpu.CompilerParams(vmem_limit_bytes=4 * 1024 * 1024),
    )(landed)


def solution(mesh):
    spec = P(("blk", "seq"), None)
    return jax.shard_map(
        on_device, mesh=mesh, in_specs=(spec,) * 3, out_specs=spec, check_vma=False
    )
```
